256 devices in a mesh: row: 16 (over y, x), col: 4 (over z_lo), depth: 4 (over z_hi, core).
Axes of the slice: x: 4, y: 4, z: 8 (z_hi: 2, z_lo: 4; z = z_hi * 4 + z_lo), core: 2. Of those that a mesh axis runs over, the one named last changes fastest.
Arguments:
- spd_matrix: float32 [16384, 16384], P('row', ('col', 'depth')), may hold values from -8 to 24
Outputs:
- panel_factor: float32 [16384, 512], P('row')
- schur_part: float32 [16384, 16384], P('row', ('col', 'depth'))
The draws below stay inside these ranges and needn't reach their ends.
All inputs are finite; a program needn't handle non-finite values.
Results may differ from the reference program's by a relative error of at most 0.00015.
Values sent between devices are 32-bit elements; how exact they have to be, the bound alone decides.
A program may use at most 64 MiB of HBM per device.

```python
import math
import jax
import jax.numpy as jnp
from jax import lax

ORDER = 16384
PANEL = 512


def draw_spd_matrix(key, part):
    first = jax.random.fold_in(key, 11)
    second = jax.random.fold_in(key, 12)
    third = jax.random.fold_in(key, 13)
    loads = jnp.clip(jax.random.normal(first, (ORDER, PANEL), jnp.float32), -6.0, 6.0)
    noise = jnp.clip(jax.random.normal(second, (ORDER, ORDER), jnp.float32), -6.0, 6.0)
    diagonal = jax.random.uniform(third, (ORDER,), jnp.float32, 3.0, 5.0)
    loads = loads * math.sqrt(3.0 / PANEL)
    noise = noise * (0.5 / math.sqrt(ORDER))
    gram = jnp.dot(loads, loads.T, precision=lax.Precision.HIGHEST, preferred_element_type=jnp.float32)
    gram = (gram + gram.T) * 0.5
    return noise + noise.T + gram + jnp.diag(diagonal)


def setup_inputs(seed: int = 0) -> dict:
    arg_keys = jax.random.split(jax.random.key(seed), 2)
    spd_matrix = draw_spd_matrix(jax.random.fold_in(arg_keys[1], 71), 0)
    return {"spd_matrix": spd_matrix}


def reference(spd_matrix):
    pivot = spd_matrix[:PANEL, :PANEL]
    pivot_factor = jnp.linalg.cholesky(pivot)
    panel_factor = lax.linalg.triangular_solve(pivot_factor, spd_matrix[:, :PANEL], left_side=False, lower=True, transpose_a=True)
    update = lax.dot_general(panel_factor.astype(jnp.float32), panel_factor.astype(jnp.float32), (((1,), (1,)), ((), ())), precision=lax.Precision.HIGHEST, preferred_element_type=jnp.float32)
    return (panel_factor, spd_matrix - update)
```

```python
import functools

import jax
import jax.numpy as jnp
from jax import lax
from jax.experimental import pallas as pl
from jax.experimental.pallas import tpu as pltpu
from jax.sharding import PartitionSpec as P

PANEL = 512
NB = 128
NP = PANEL // NB
K = 16
HOP = 3
HI = lax.Precision.HIGHEST
F32 = jnp.float32


def dot(a, b, ca, cb):
    return lax.dot_general(
        a, b, (((ca,), (cb,)), ((), ())), precision=HI, preferred_element_type=F32
    )


def lane(a, k):
    return jnp.broadcast_to(a[:, k : k + 1], (8, NB))


def sub(a, i):
    return jnp.broadcast_to(a[i : i + 1, :], a.shape)


def factor_block(M, W, look=2):
    rows = lax.broadcasted_iota(jnp.int32, (8, NB), 0)
    steps = NB // 8
    for t in range(steps):
        blocks = list(range(t, min(t + look + 1, steps)))
        R = [M[8 * s : 8 * s + 8, 0:NB] for s in blocks]
        E = [M[8 * s : 8 * s + 8, NB : 2 * NB] for s in blocks]
        C = [[lane(r, 8 * t + i) for i in range(8)] for r in R]
        d = jnp.zeros((8, NB), F32)
        for i in range(8):
            own = C[0][i]
            d = jnp.where(rows == i, own, d)
            inv = 1.0 / sub(own, i)
            f = [jnp.where(rows > i, own, 0.0) * inv]
            f += [C[b][i] * inv for b in range(1, len(blocks))]
            for j in range(i + 1, 8):
                g = sub(C[0][j], i)
                for b in range(len(blocks)):
                    C[b][j] = C[b][j] - f[b] * g
            gr, ge = sub(R[0], i), sub(E[0], i)
            for b in range(len(blocks)):
                R[b] = R[b] - f[b] * gr
                E[b] = E[b] - f[b] * ge
        s = lax.rsqrt(d)
        u, v = R[0] * s, E[0] * s
        W[8 * t : 8 * t + 8, :] = v
        for b in range(1, len(blocks)):
            r = 8 * blocks[b]
            M[r : r + 8, 0:NB] = R[b]
            M[r : r + 8, NB : 2 * NB] = E[b]
        lo = 8 * (t + look + 1)
        if lo < NB:
            upd = dot(u, jnp.concatenate([u, v], axis=1), 0, 0)
            M[lo:NB, :] = M[lo:NB, :] - upd[lo:NB, :]


def factor_step(S, F, M, p):
    a, b = p * NB, (p + 1) * NB
    eye = lax.broadcasted_iota(jnp.int32, (NB, NB), 0) == lax.broadcasted_iota(
        jnp.int32, (NB, NB), 1
    )
    M[:, 0:NB] = S[a:b, a:b]
    M[:, NB : 2 * NB] = eye.astype(F32)
    factor_block(M, F.at[a:b, a:b])
    if p < NP - 1:
        u = dot(F[a:b, a:b], S[a:b, b:], 1, 0)
        F[a:b, b:] = u
        S[b:, b:] = S[b:, b:] - dot(u, u, 0, 0)


def place():
    row, col, depth = (lax.axis_index(a) for a in ("row", "col", "depth"))
    y, x = row // 4, row % 4
    z, core = (depth // 2) * 4 + col, depth % 2
    return y, x, z, core


def device(y, x, z, core):
    return (y * 4 + x, z % 4, (z // 4) * 2 + core)


def share(a_ref, x_ref, r_ref, f_ref, S, M, x_send, x_recv, z_send, z_recv, d_send, d_recv, m_send, m_recv, load):
    y, x, z, core = place()
    other = 1 - core
    xsrc = (y == 0) & (x == 0)
    rsrc = (z == 0) & (core == 0)
    root = xsrc & rsrc

    load_x = pltpu.make_async_copy(a_ref.at[0:PANEL, :], x_ref, load.at[0])
    load_r = pltpu.make_async_copy(a_ref.at[:, 0:PANEL], r_ref, load.at[1])

    @pl.when(xsrc)
    def _():
        load_x.start()

    @pl.when(rsrc)
    def _():
        load_r.start()

    barrier = pltpu.get_barrier_semaphore()
    peers = [device(y, (x + i) % 4, z, core) for i in (1, 2, 3)]
    peers += [device((y + i) % 4, x, z, core) for i in (1, 2, 3)]
    peers += [device(y, x, (z + i) % 8, core) for i in (1, 2, 6, 7)]
    peers += [device(y, x, z, other)]
    for peer in peers:
        pl.semaphore_signal(barrier, inc=1, device_id=peer, device_id_type=pl.DeviceIdType.MESH)
    pl.semaphore_wait(barrier, len(peers))

    @pl.when(xsrc)
    def _():
        load_x.wait()

    @pl.when(rsrc)
    def _():
        load_r.wait()

    def remote(src, dst, send, recv, to):
        return pltpu.make_async_remote_copy(
            src_ref=src, dst_ref=dst, send_sem=send, recv_sem=recv,
            device_id=to, device_id_type=pl.DeviceIdType.MESH,
        )

    trees = []
    for tree in range(4):
        step = 1 if tree < 2 else 3
        v, u = (y, x) if tree < 2 else ((4 - y) % 4, (4 - x) % 4)
        if tree % 2:
            v, u = u, v
        along = ((v == 0) & (u < 3)) | ((v > 0) & (u == 3))
        across = (u > 0) & (v < 3)
        depth = jnp.where((u == 0) & (v > 0), v + 4, u + v)
        to_along = device(y, (x + step) % 4, z, core)
        to_across = device((y + step) % 4, x, z, core)
        if tree % 2:
            to_along, to_across = to_across, to_along
        trees.append((depth * HOP, ((along, to_along), (across, to_across))))

    def x_part(tree, k):
        return x_ref.at[pl.ds(pl.multiple_of(tree * 128 + k * 8, 8), 8), :]

    def x_copy(tree, child, k):
        part = x_part(tree, k)
        return remote(part, part, x_send.at[tree, child, k], x_recv.at[tree, k], trees[tree][1][child][1])

    half = PANEL

    def r_part(which, k):
        return r_ref.at[pl.ds(pl.multiple_of(which * half + k * 32, 32), 32), :]

    z_depth = jnp.where(core == 0, z * HOP, ((8 - z) % 8 + 1) * HOP)
    z_on = jnp.where(core == 0, z < 7, z != 1)
    z_to = device(y, x, jnp.where(core == 0, (z + 1) % 8, (z + 7) % 8), core)
    z_gets = jnp.logical_not(rsrc)
    gives = (z > 0) | (core == 0)
    partner = device(y, x, z, other)

    def z_copy(k):
        part = r_part(core, k)
        return remote(part, part, z_send.at[k], z_recv.at[k], z_to)

    def d_copy(k):
        part = r_part(core, k)
        return remote(part, part, d_send.at[0, k], d_recv.at[k], partner)

    def d_first(k):
        part = r_part(other, k)
        return remote(part, part, d_send.at[1, k], z_recv.at[k], partner)

    def slot(t, _):
        for tree in range(4):
            start, children = trees[tree]
            k = t - start

            @pl.when((k >= 0) & (k < K))
            def _(tree=tree, children=children, k=k):
                @pl.when(jnp.logical_not(xsrc))
                def _():
                    x_copy(tree, 0, k).wait_recv()

                for child in range(2):
                    @pl.when(children[child][0])
                    def _(child=child):
                        x_copy(tree, child, k).start()

        k = t - z_depth

        @pl.when((k >= 0) & (k < K))
        def _():
            @pl.when(z_gets)
            def _():
                z_copy(k).wait_recv()

            @pl.when(rsrc)
            def _():
                d_first(k).start()

            @pl.when(z_on)
            def _():
                z_copy(k).start()

            @pl.when(gives)
            def _():
                d_copy(k).start()

        return 0

    lax.fori_loop(0, K + 8 * HOP, slot, 0)

    zline = xsrc & (core == 0)
    xline = (y == 0) & (core == 0)
    routes = [
        (zline & (z == 0), device(y, x, 2, core)),
        (zline & (z == 0), device(y, x, 6, core)),
        (zline & (z == 0), device(y, x, 1, core)),
        (zline & (z == 0), device(y, x, 7, core)),
        (zline & (z == 2), device(y, x, 4, core)),
        (zline & (z == 2), device(y, x, 3, core)),
        (zline & (z == 6), device(y, x, 5, core)),
    ]
    routes += [(xline & (x == 0), device(y, i, z, core)) for i in (2, 1, 3)]
    routes += [((y == 0) & (core == 0), device(i, x, z, core)) for i in (2, 1, 3)]
    routes += [(core == 0, partner)]

    def m_copy(p, i, to):
        part = f_ref.at[NB * p : NB * (p + 1), NB * p : PANEL]
        return remote(part, part, m_send.at[p, i], m_recv.at[p], to)

    def forward(p):
        for i, (here, to) in enumerate(routes):
            @pl.when(here)
            def _(i=i, to=to):
                m_copy(p, i, to).start()

    @pl.when(root)
    def _():
        S[...] = r_ref[0:PANEL, :]
        for p in range(NP):
            factor_step(S, f_ref, M, p)
            forward(p)

    @pl.when(jnp.logical_not(root))
    def _():
        for p in range(NP):
            m_copy(p, 0, partner).wait_recv()
            forward(p)

    for p in range(NP):
        for i, (here, to) in enumerate(routes):
            @pl.when(here)
            def _(p=p, i=i, to=to):
                m_copy(p, i, to).wait_send()

    def drain(k, _):
        for tree in range(4):
            for child in range(2):
                @pl.when(trees[tree][1][child][0])
                def _(tree=tree, child=child):
                    x_copy(tree, child, k).wait_send()

        @pl.when(z_on)
        def _():
            z_copy(k).wait_send()

        @pl.when(gives)
        def _():
            d_copy(k).wait_send()

        @pl.when(rsrc)
        def _():
            d_first(k).wait_send()

        @pl.when(jnp.where(core == 0, z > 0, True))
        def _():
            pltpu.make_async_copy(r_part(other, k), r_part(other, k), d_recv.at[k]).wait()

        return 0

    lax.fori_loop(0, K, drain, 0)


def finish(a_ref, r_ref, x_ref, f_ref, panel_ref, out_ref, Y, Z):
    def block(p, q):
        return f_ref[NB * p : NB * (p + 1), NB * q : NB * (q + 1)]

    @pl.when(pl.program_id(0) == 0)
    def _():
        for p in range(NP):
            acc = x_ref[NB * p : NB * (p + 1), :]
            if p:
                acc = acc - dot(f_ref[0 : NB * p, NB * p : NB * (p + 1)], Y[0 : NB * p, :], 0, 0)
            Y[NB * p : NB * (p + 1), :] = dot(block(p, p), acc, 1, 0)

    for p in range(NP):
        acc = r_ref[:, NB * p : NB * (p + 1)]
        if p:
            acc = acc - dot(Z[:, 0 : NB * p], f_ref[0 : NB * p, NB * p : NB * (p + 1)], 1, 0)
        Z[:, NB * p : NB * (p + 1)] = dot(acc, block(p, p), 1, 1)
    panel_ref[...] = Z[...]
    out_ref[...] = a_ref[...] - dot(Z[...], Y[...], 1, 0)


def step(a):
    rows, cols = a.shape
    vmem = pl.BlockSpec(memory_space=pltpu.VMEM)
    x, r, f = pl.pallas_call(
        share,
        name="share",
        out_shape=(
            jax.ShapeDtypeStruct((PANEL, cols), F32),
            jax.ShapeDtypeStruct((rows, PANEL), F32),
            jax.ShapeDtypeStruct((PANEL, PANEL), F32),
        ),
        in_specs=[pl.BlockSpec(memory_space=pl.ANY)],
        out_specs=(vmem, vmem, vmem),
        scratch_shapes=[
            pltpu.VMEM((PANEL, PANEL), F32),
            pltpu.VMEM((NB, 2 * NB), F32),
            pltpu.SemaphoreType.DMA((4, 2, K)),
            pltpu.SemaphoreType.DMA((4, K)),
            pltpu.SemaphoreType.DMA((K,)),
            pltpu.SemaphoreType.DMA((K,)),
            pltpu.SemaphoreType.DMA((2, K)),
            pltpu.SemaphoreType.DMA((K,)),
            pltpu.SemaphoreType.DMA((NP, 14)),
            pltpu.SemaphoreType.DMA((NP,)),
            pltpu.SemaphoreType.DMA((2,)),
        ],
        compiler_params=pltpu.CompilerParams(collective_id=0, has_side_effects=True, vmem_limit_bytes=24 << 20),
    )(a)
    tile = 128
    full = lambda shape: pl.BlockSpec(shape, lambda i: (0, 0))
    return pl.pallas_call(
        finish,
        name="finish",
        grid=(rows // tile,),
        out_shape=(
            jax.ShapeDtypeStruct((rows, PANEL), F32),
            jax.ShapeDtypeStruct((rows, cols), F32),
        ),
        in_specs=[
            pl.BlockSpec((tile, cols), lambda i: (i, 0)),
            pl.BlockSpec((tile, PANEL), lambda i: (i, 0)),
            full((PANEL, cols)),
            full((PANEL, PANEL)),
        ],
        out_specs=(
            pl.BlockSpec((tile, PANEL), lambda i: (i, 0)),
            pl.BlockSpec((tile, cols), lambda i: (i, 0)),
        ),
        scratch_shapes=[pltpu.VMEM((PANEL, cols), F32), pltpu.VMEM((tile, PANEL), F32)],
        compiler_params=pltpu.CompilerParams(vmem_limit_bytes=24 << 20),
    )(a, r, x, f)


def solution(mesh):
    placed = P("row", ("col", "depth"))
    return jax.shard_map(
        step, mesh=mesh, in_specs=(placed,), out_specs=(P("row", None), placed), check_vma=False
    )
```
